256 devices in a mesh: dp: 32 (over z, y_lo, core), grp: 8 (over x, y_hi).
Axes of the slice: x: 4, y: 4 (y_hi: 2, y_lo: 2; y = y_hi * 2 + y_lo), z: 8, core: 2. Of those that a mesh axis runs over, the one named last changes fastest.
Arguments:
- acts: bfloat16 [131072, 1024], P(('dp', 'grp')), may hold values from -8 to 8, as said below
- grads: bfloat16 [131072, 1024], P(('dp', 'grp')), may hold values from -8 to 8, as said below
- damping: float32 [2], replicated, may hold values from 0.02 to 0.2
Outputs:
- preconditioned: float32 [1024, 1024], P('dp', 'grp')
The draws below stay inside these ranges and needn't reach their ends.
Inputs may be any that keep to these rules, and one draw needn't show every extreme that they name: `acts`: activations of one token are correlated across features. `grads`: output gradients are correlated with the activations.
All inputs are finite; a program needn't handle non-finite values. Where the reference program divides by a largest or mean magnitude, that divisor is 1e-20 or more.
Results may differ from the reference program's by a relative error of at most 0.0003.
Values sent between devices are 32-bit elements; how exact they have to be, the bound alone decides.
No kernel may reach another device: no remote copies, remote signals or barrier semaphores. Data moves between devices by JAX's collectives and lax.ppermute only.
A program may use at most 64 MiB of HBM per device.

```python
import math
import jax
import jax.numpy as jnp
from jax import lax

D = 1024
ITERS = 4
TOKENS = 131072


def base_acts(key):
    inner = jax.random.fold_in(key, 101)
    key_noise, key_mix, key_scale = jax.random.split(inner, 3)
    noise = jax.random.normal(key_noise, (TOKENS, D), jnp.float32)
    mixing = jnp.eye(D, dtype=jnp.float32) + 0.5 * jax.random.normal(key_mix, (D, D), jnp.float32) / math.sqrt(D)
    scales = jnp.exp(jax.random.uniform(key_scale, (D,), jnp.float32, math.log(0.1), 0.0))
    return jnp.dot(noise, mixing, precision=lax.Precision.HIGHEST) * scales


def draw_acts(key, part):
    return jnp.clip(base_acts(key), -8.0, 8.0).astype(jnp.bfloat16)


def draw_grads(key, part):
    values = base_acts(key)
    inner = jax.random.fold_in(key, 202)
    key_cross, key_noise, key_scale = jax.random.split(inner, 3)
    coupling = jax.random.normal(key_cross, (D, D), jnp.float32) / math.sqrt(D)
    noise = jax.random.normal(key_noise, (TOKENS, D), jnp.float32)
    scales = jnp.exp(jax.random.uniform(key_scale, (D,), jnp.float32, math.log(0.1), 0.0))
    result = jnp.dot(values, coupling, precision=lax.Precision.HIGHEST) + noise * scales
    return jnp.clip(result, -8.0, 8.0).astype(jnp.bfloat16)


def setup_inputs(seed: int = 0) -> dict:
    key_of = jax.random.split(jax.random.key(seed), 4)
    return {
        "acts": draw_acts(jax.random.fold_in(key_of[3], 71), 0),
        "grads": draw_grads(jax.random.fold_in(key_of[3], 71), 0),
        "damping": jnp.clip(jnp.exp(jax.random.uniform(key_of[2], (2,), jnp.float32, math.log(0.02), math.log(0.2))), 0.02, 0.2),
    }


def newton_inverse(gram, damp):
    size = gram.shape[0]
    eye = jnp.eye(size, dtype=jnp.float32)
    matrix = gram + damp * eye
    alpha = 1.0 / jnp.max(jnp.sum(jnp.abs(matrix), axis=1))
    iterate = alpha * eye
    for step in range(ITERS):
        image = jnp.dot(matrix, iterate, precision=lax.Precision.HIGHEST)
        iterate = 2.0 * iterate - jnp.dot(iterate, image, precision=lax.Precision.HIGHEST)
    return iterate


def reference(acts, grads, damping):
    contract = (((0,), (0,)), ((), ()))
    scale = 1.0 / TOKENS
    gram_acts = lax.dot_general(acts, acts, contract, preferred_element_type=jnp.float32) * scale
    gram_grads = lax.dot_general(grads, grads, contract, preferred_element_type=jnp.float32) * scale
    left = newton_inverse(gram_acts, damping[0])
    right = newton_inverse(gram_grads, damping[1])
    mapped = jnp.dot(acts.astype(jnp.float32), left, precision=lax.Precision.HIGHEST)
    weighted = jnp.dot(grads.astype(jnp.float32), right, precision=lax.Precision.HIGHEST)
    return lax.dot_general(mapped, weighted, contract, precision=lax.Precision.HIGHEST, preferred_element_type=jnp.float32) * scale
```

```python
import functools

import jax
import jax.numpy as jnp
from jax import lax
from jax.experimental import pallas as pl
from jax.experimental.pallas import tpu as pltpu
from jax.sharding import Mesh
from jax.sharding import PartitionSpec as P

INTERPRET = False
STEPS = 14
AXES = ("zh", "zl", "yl", "c", "x", "yh")
DP = ("zh", "zl", "yl", "c")
GRP = ("x", "yh")
RING = ("zl", "yl", "x", "yh")
B = 128
F32 = jnp.float32
BF16 = jnp.bfloat16


def sub_segments(start, size, piece):
    done = 0
    while done < size:
        q, r = divmod(start + done, piece)
        n = min(piece - r, size - done)
        yield q, r, done, n
        done += n


def dot(a, b):
    return jnp.dot(a, b, preferred_element_type=F32)


def gram_kernel(nb, nq, ng, core_ref, acts_ref, grads_ref, keep_ref, send_ref, t_ref):
    core = core_ref[0]
    width = nb * B
    half = width // 2
    piece = nb * (nb + 1) // 2 * B // nq
    acts = acts_ref[...]
    grads = grads_ref[...]
    for which, out in ((0, send_ref), (1, keep_ref)):
        own = (core == 0) if which else (core != 0)
        part = jnp.where(own, acts, grads)
        t_ref[...] = part.T
        for jj in range(nb // 2):
            cols = part[:, jj * 2 * B : (jj + 1) * 2 * B]
            res = dot(t_ref[: (jj + 1) * 2 * B, :], cols)
            for j in (2 * jj, 2 * jj + 1):
                lane = (j - 2 * jj) * B
                for q, r, at, n in sub_segments(j * (j + 1) // 2 * B, (j + 1) * B, piece):
                    out[q, r : r + n, :] = res[at : at + n, lane : lane + B]
    t_ref[...] = acts.T
    runs = half // 32
    for which, out in ((0, send_ref), (1, keep_ref)):
        first = core * half if which else (1 - core) * half
        rows = t_ref[pl.ds(pl.multiple_of(first, half), half), :]
        for jj in range(nb // 2):
            res = dot(rows, grads[:, jj * 2 * B : (jj + 1) * 2 * B])
            for s in range(runs):
                zh, rest = divmod(s, runs // 4)
                for k in range(2):
                    q = rest * ng + 2 * jj + k
                    out[q, piece + zh * 32 : piece + zh * 32 + 32, :] = res[s * 32 : s * 32 + 32, k * B : k * B + B]


def split(v):
    hi = v.astype(BF16)
    return hi, (v - hi.astype(F32)).astype(BF16)


def inverse_kernel(nb, scale, start_ref, damp_ref, packed_ref, out_ref, m_ref, hi_ref, lo_ref, s_ref, y_ref):
    width = nb * B
    damp = damp_ref[0]
    eye = (lax.broadcasted_iota(jnp.int32, (B, B), 0) == lax.broadcasted_iota(jnp.int32, (B, B), 1)).astype(F32)
    for j in range(nb):
        base = j * (j + 1) // 2 * B
        for i in range(j + 1):
            block = packed_ref[base + i * B : base + (i + 1) * B, :] * scale
            if i == j:
                block = block + damp * eye
            m_ref[i * B : (i + 1) * B, j * B : (j + 1) * B] = block
            if i != j:
                m_ref[j * B : (j + 1) * B, i * B : (i + 1) * B] = block.T
    total = jnp.zeros((8, width), F32)
    for i in range(nb):
        total = total + jnp.abs(m_ref[i * B : (i + 1) * B, :]).reshape(B // 8, 8, width).sum(axis=0)
    alpha = 1.0 / jnp.max(jnp.sum(total, axis=0, keepdims=True), axis=1, keepdims=True)
    for i in range(nb):
        rows = lax.broadcasted_iota(jnp.int32, (B, width), 0) + i * B
        ones = (rows == lax.broadcasted_iota(jnp.int32, (B, width), 1)).astype(F32)
        hi, lo = split(ones - alpha * m_ref[i * B : (i + 1) * B, :])
        hi_ref[i * B : (i + 1) * B, :] = hi
        lo_ref[i * B : (i + 1) * B, :] = lo
    start = pl.multiple_of(start_ref[0], B)
    rows = lax.broadcasted_iota(jnp.int32, (B, width), 0) + start
    ones = (rows == lax.broadcasted_iota(jnp.int32, (B, width), 1)).astype(F32)
    s_ref[...] = ones
    y_ref[...] = 2.0 * ones - alpha * m_ref[pl.ds(start, B), :]

    def step(_, carry):
        hi, lo = split(y_ref[...])
        both = jnp.concatenate([hi, lo], axis=0)
        first = dot(both, hi_ref[...])
        y_ref[...] = (dot(hi, lo_ref[...]) + first[B:]) + first[:B] + s_ref[...]
        return carry

    lax.fori_loop(0, STEPS, step, 0)
    out_ref[...] = alpha * y_ref[...]


def vmem(n):
    return [pl.BlockSpec(memory_space=pltpu.VMEM)] * n


def smem():
    return pl.BlockSpec(memory_space=pltpu.SMEM)


def gram_pieces(acts, grads, core, nq, ng):
    tokens, width = acts.shape
    nb = width // B
    piece = nb * (nb + 1) // 2 * B // nq
    cross = width // 2 * width // nq // B
    shape = jax.ShapeDtypeStruct((nq, piece + cross, B), F32)
    return pl.pallas_call(
        functools.partial(gram_kernel, nb, nq, ng),
        out_shape=[shape, shape],
        in_specs=[smem()] + vmem(2),
        out_specs=vmem(2),
        scratch_shapes=[pltpu.VMEM((width, tokens), BF16)],
        name="grams",
        interpret=INTERPRET,
    )(core[None], acts, grads)


def inverse_rows(packed, damp, start, nb, scale):
    width = nb * B
    return pl.pallas_call(
        functools.partial(inverse_kernel, nb, scale),
        out_shape=jax.ShapeDtypeStruct((B, width), F32),
        in_specs=[smem(), smem()] + vmem(1),
        out_specs=vmem(1)[0],
        scratch_shapes=[
            pltpu.VMEM((width, width), F32),
            pltpu.VMEM((width, width), BF16),
            pltpu.VMEM((width, width), BF16),
            pltpu.VMEM((B, width), F32),
            pltpu.VMEM((B, width), F32),
        ],
        cost_estimate=pl.CostEstimate(
            flops=2 * 3 * STEPS * B * width * width, bytes_accessed=4 * width * width, transcendentals=0
        ),
        name="inverse",
        interpret=INTERPRET,
    )(start[None], damp[None], packed)


def everywhere(array, axes):
    size = lax.axis_size(axes)
    return lax.all_to_all(jnp.broadcast_to(array[None], (size, *array.shape)), axes, 0, 0, tiled=True)


def swapped(array):
    return lax.ppermute(array, "c", [(0, 1), (1, 0)])


def local(acts, grads, damping):
    tokens, width = acts.shape
    nb = width // B
    nq, ng = lax.axis_size(RING), lax.axis_size(GRP)
    nz = lax.axis_size("zh")
    scale = 1.0 / (tokens * lax.axis_size(AXES))
    core = lax.axis_index("c")
    keep, send = gram_pieces(acts, grads, core, nq, ng)
    chip = keep + swapped(send)
    piece = nb * (nb + 1) // 2 * B // nq
    plane = lax.all_to_all(chip, RING, 0, 0, tiled=True).sum(axis=0)
    factor, cross = plane[:piece], plane[piece:].reshape(nz, -1, B)
    mixed = jnp.concatenate([jnp.broadcast_to(factor[None], (nz, *factor.shape)), cross], axis=1)
    whole = lax.all_to_all(mixed, "zh", 0, 0, tiled=True).sum(axis=0)
    factor, cross = whole[:piece], whole[piece:]
    packed = everywhere(factor, RING).reshape(-1, B)
    cross_rows = everywhere(cross, GRP)
    height = lax.axis_index("zh") * lax.axis_size("zl") + lax.axis_index("zl")
    start = jnp.where(core == 0, height * B, lax.axis_index(GRP) * B).astype(jnp.int32)
    damp = jnp.where(core == 0, damping[0], damping[1])
    mine = inverse_rows(packed, damp, start, nb, scale)
    other = swapped(mine)
    left = jnp.where(core == 0, mine, other)
    right = jnp.where(core == 0, other, mine)
    highest = lax.Precision.HIGHEST
    right_blocks = right.reshape(B, ng, B)
    z = jnp.einsum("grk,cgk->rc", cross_rows * scale, right_blocks, precision=highest, preferred_element_type=F32)
    z_all = everywhere(z, DP)
    z_all = z_all.reshape(-1, 2, *z.shape).swapaxes(0, 1).reshape(width, B)
    rows = z.shape[0]
    first = lax.axis_index("yl") * 2 * rows + core * rows
    left_rows = lax.dynamic_slice_in_dim(left, first, rows, 0)
    return jnp.dot(left_rows, z_all, precision=highest, preferred_element_type=F32)


def solution(mesh):
    torus = Mesh(mesh.devices.reshape(4, 2, 2, 2, 4, 2), AXES)
    return jax.shard_map(
        local,
        mesh=torus,
        in_specs=(P(AXES, None), P(AXES, None), P()),
        out_specs=P(DP, GRP),
        check_vma=False,
    )
```

```python
import functools
import math

import jax
import jax.numpy as jnp
from jax import lax
from jax.experimental import pallas as pl
from jax.experimental.pallas import tpu as pltpu
from jax.sharding import Mesh
from jax.sharding import PartitionSpec as P

INTERPRET = False
STEPS = 14
AXES = ("zh", "zl", "yl", "c", "x", "yh")
DP = ("zh", "zl", "yl", "c")
GRP = ("x", "yh")
PLANE = ("yl", "x", "yh")
RING = ("zl", "yl", "x", "yh")
B = 128
F32 = jnp.float32
BF16 = jnp.bfloat16


def sub_segments(start, size, piece):
    done = 0
    while done < size:
        q, r = divmod(start + done, piece)
        n = min(piece - r, size - done)
        yield q, r, done, n
        done += n


def dot(a, b):
    return jnp.dot(a, b, preferred_element_type=F32)


def factor_kernel(nb, nq, core_ref, acts_ref, grads_ref, keep_ref, send_ref, t_ref):
    core = core_ref[0]
    piece = nb * (nb + 1) // 2 * B // nq
    acts = acts_ref[...]
    grads = grads_ref[...]
    for which, out in ((0, send_ref), (1, keep_ref)):
        own = (core == 0) if which else (core != 0)
        part = jnp.where(own, acts, grads)
        t_ref[...] = part.T
        for jj in range(nb // 2):
            cols = part[:, jj * 2 * B : (jj + 1) * 2 * B]
            res = dot(t_ref[: (jj + 1) * 2 * B, :], cols)
            for j in (2 * jj, 2 * jj + 1):
                lane = (j - 2 * jj) * B
                for q, r, at, n in sub_segments(j * (j + 1) // 2 * B, (j + 1) * B, piece):
                    out[q, r : r + n, :] = res[at : at + n, lane : lane + B]


def cross_kernel(nb, nz, ng, core_ref, acts_ref, grads_ref, keep_ref, send_ref, t_ref):
    core = core_ref[0]
    half = nb * B // 2
    grads = grads_ref[...]
    t_ref[...] = acts_ref[...].T
    rows = keep_ref.shape[2]
    runs = half // rows
    for which, out in ((0, send_ref), (1, keep_ref)):
        first = core * half if which else (1 - core) * half
        part = t_ref[pl.ds(pl.multiple_of(first, half), half), :]
        for jj in range(nb // 2):
            res = dot(part, grads[:, jj * 2 * B : (jj + 1) * 2 * B])
            for s in range(runs):
                zh, rest = divmod(s, runs // nz)
                for k in range(2):
                    out[zh, rest * ng + 2 * jj + k, :, :] = res[s * rows : s * rows + rows, k * B : k * B + B]


def turned_add_kernel(nz, at_ref, keep_ref, came_ref, *outs):
    for k, out in enumerate(outs):
        z = lax.rem(at_ref[0] + k, nz)
        out[...] = keep_ref[z] + came_ref[z]


def halves_kernel(at_ref, pieces_ref, keep_ref, send_ref, sum_ref):
    total = pieces_ref[0]
    for k in range(1, pieces_ref.shape[0]):
        total = total + pieces_ref[k]
    sum_ref[...] = total
    size = keep_ref.shape[0]
    at = at_ref[0]
    keep_ref[...] = sum_ref[pl.ds(pl.multiple_of(at * size, 8), size), :]
    send_ref[...] = sum_ref[pl.ds(pl.multiple_of((1 - at) * size, 8), size), :]


def outgoing_kernel(*refs):
    out = refs[-1]
    count = (len(refs) - 1) // 2
    factor = refs[0][...]
    for ref in refs[1:count]:
        factor = factor + ref[...]
    piece = factor.shape[0]
    for q in range(out.shape[0]):
        out[q, :piece, :] = factor
        cross = refs[count][q]
        for ref in refs[count + 1 : 2 * count]:
            cross = cross + ref[q]
        out[q, piece:, :] = cross


def last_kernel(at_ref, mine_ref, other_ref, *refs):
    out_ref, z_ref = refs[-2:]
    core, zl, yl = at_ref[0], at_ref[1], at_ref[2]
    own, came = refs[:4], refs[4]
    for d in range(4):
        dz, dy = divmod(d, 2)
        pz, py = jnp.bitwise_xor(zl, dz), jnp.bitwise_xor(yl, dy)
        for zh in range(z_ref.shape[1]):
            z_ref[core, zh, pz, py] = own[d][zh]
            z_ref[1 - core, zh, pz, py] = came[d, zh]
    rows = out_ref.shape[0]
    first = pl.multiple_of(yl * 2 * rows + core * rows, 8)
    mine = mine_ref[pl.ds(first, rows), :]
    other = other_ref[pl.ds(first, rows), :]
    hi, lo = split(jnp.where(core == 0, mine, other))
    zhi, zlo = split(z_ref[...].reshape(-1, B))
    out_ref[...] = (dot(hi, zlo) + dot(lo, zhi)) + dot(hi, zhi)


def split(v):
    hi = v.astype(BF16)
    return hi, (v - hi.astype(F32)).astype(BF16)


def inverse_kernel(nb, nq, scale, start_ref, damp_ref, packed_ref, out_ref, m_ref, hi_ref, lo_ref, s_ref, y_ref):
    width = nb * B
    damp = damp_ref[0]
    eye = (lax.broadcasted_iota(jnp.int32, (B, B), 0) == lax.broadcasted_iota(jnp.int32, (B, B), 1)).astype(F32)
    piece = nb * (nb + 1) // 2 * B // (2 * nq)
    for j in range(nb):
        base = j * (j + 1) // 2 * B
        for i in range(j + 1):
            parts = []
            for q, r, _, n in sub_segments(base + i * B, B, piece):
                parts.append(packed_ref[q % 2 * nq + q // 2, r : r + n, :])
            block = jnp.concatenate(parts, axis=0) * scale
            if i == j:
                block = block + damp * eye
            m_ref[i * B : (i + 1) * B, j * B : (j + 1) * B] = block
            if i != j:
                m_ref[j * B : (j + 1) * B, i * B : (i + 1) * B] = block.T
    total = jnp.zeros((8, width), F32)
    for i in range(nb):
        total = total + jnp.abs(m_ref[i * B : (i + 1) * B, :]).reshape(B // 8, 8, width).sum(axis=0)
    alpha = 1.0 / jnp.max(jnp.sum(total, axis=0, keepdims=True), axis=1, keepdims=True)
    for i in range(nb):
        rows = lax.broadcasted_iota(jnp.int32, (B, width), 0) + i * B
        ones = (rows == lax.broadcasted_iota(jnp.int32, (B, width), 1)).astype(F32)
        hi, lo = split(ones - alpha * m_ref[i * B : (i + 1) * B, :])
        hi_ref[i * B : (i + 1) * B, :] = hi
        lo_ref[i * B : (i + 1) * B, :] = lo
    start = pl.multiple_of(start_ref[0], B)
    rows = lax.broadcasted_iota(jnp.int32, (B, width), 0) + start
    ones = (rows == lax.broadcasted_iota(jnp.int32, (B, width), 1)).astype(F32)
    s_ref[...] = ones
    y_ref[...] = 2.0 * ones - alpha * m_ref[pl.ds(start, B), :]

    def step(_, carry):
        hi, lo = split(y_ref[...])
        both = jnp.concatenate([hi, lo], axis=0)
        first = dot(both, hi_ref[...])
        y_ref[...] = (dot(hi, lo_ref[...]) + first[B:]) + first[:B] + s_ref[...]
        return carry

    lax.fori_loop(0, STEPS, step, 0)
    out_ref[...] = alpha * y_ref[...]


def vmem(n):
    return [pl.BlockSpec(memory_space=pltpu.VMEM)] * n


def smem(n=1):
    return [pl.BlockSpec(memory_space=pltpu.SMEM)] * n


def call(kernel, scalars, arrays, outs, scratch=(), flops=0, limit=32):
    moved = sum(4 * math.prod(o) for o in outs) + sum(a.size * a.dtype.itemsize for a in arrays)
    shapes = [jax.ShapeDtypeStruct(o, F32) for o in outs]
    return pl.pallas_call(
        kernel,
        out_shape=shapes,
        in_specs=smem(len(scalars)) + vmem(len(arrays)),
        out_specs=vmem(len(outs)),
        scratch_shapes=list(scratch),
        cost_estimate=pl.CostEstimate(flops=flops, bytes_accessed=moved, transcendentals=0),
        compiler_params=pltpu.CompilerParams(vmem_limit_bytes=limit << 20),
        interpret=INTERPRET,
    )(*[jnp.atleast_1d(s) for s in scalars], *arrays)


def everywhere(array, axes):
    size = lax.axis_size(axes)
    return lax.all_to_all(jnp.broadcast_to(array[None], (size, *array.shape)), axes, 0, 0, tiled=True)


def swapped(array, axes):
    pairs = [(k, lax.axis_size(axes) - 1 - k) for k in range(lax.axis_size(axes))]
    return lax.ppermute(array, axes, pairs)


def shifted(array, axis, by):
    size = lax.axis_size(axis)
    return lax.ppermute(array, axis, [(k, (k + by) % size) for k in range(size)])


def program(acts, grads, damping):
    tokens, width = acts.shape
    nb = width // B
    nq, ng, nz = lax.axis_size(PLANE), lax.axis_size(GRP), lax.axis_size("zh")
    scale = 1.0 / (tokens * lax.axis_size(AXES))
    core, zh, zl, yl = (lax.axis_index(a) for a in ("c", "zh", "zl", "yl"))
    packed_rows = nb * (nb + 1) // 2 * B
    rows = width // lax.axis_size(DP)

    kept, sent = call(
        functools.partial(factor_kernel, nb, nq), [core], [acts, grads],
        [(nq, packed_rows // nq, B)] * 2, [pltpu.VMEM((width, tokens), BF16)], flops=2 * tokens * width * width,
    )
    cross_shape = (nz, 2 * nq, rows, B)
    cross_kept, cross_sent = call(
        functools.partial(cross_kernel, nb, nz, ng), [core], [acts, grads],
        [cross_shape] * 2, [pltpu.VMEM((width, tokens), BF16)], flops=2 * tokens * width * width,
    )
    plane = lax.all_to_all(kept + swapped(sent, "c"), PLANE, 0, 0, tiled=True)
    half_shape = (packed_rows // nq // 2, B)
    keep, send = call(halves_kernel, [zl], [plane], [half_shape] * 2, [pltpu.VMEM((2 * half_shape[0], B), F32)])
    factor = keep + swapped(send, "zl")
    factors = [factor] + [shifted(factor, "zh", k) for k in range(1, nz)]
    turned = call(
        functools.partial(turned_add_kernel, nz), [zh], [cross_kept, swapped(cross_sent, "c")],
        [cross_shape[1:]] * nz,
    )
    crosses = [turned[0]] + [shifted(turned[k], "zh", k) for k in range(1, nz)]
    (outgoing,) = call(outgoing_kernel, [], factors + crosses, [(2 * nq, half_shape[0] + rows, B)])
    pieces = lax.all_to_all(outgoing, RING, 0, 0, tiled=True)
    cross = pieces[:, half_shape[0] :, :].sum(axis=0) * scale
    cross_rows = everywhere(cross, ("zh", "x", "yh")).reshape(nz, ng, rows, B)
    height = zh * lax.axis_size("zl") + zl
    start = jnp.where(core == 0, height * B, lax.axis_index(GRP) * B).astype(jnp.int32)
    damp = jnp.where(core == 0, damping[0], damping[1])
    (mine,) = call(
        functools.partial(inverse_kernel, nb, nq, scale), [start, damp], [pieces], [(B, width)],
        [
            pltpu.VMEM((width, width), F32),
            pltpu.VMEM((width, width), BF16),
            pltpu.VMEM((width, width), BF16),
            pltpu.VMEM((B, width), F32),
            pltpu.VMEM((B, width), F32),
        ],
        flops=2 * 3 * STEPS * B * width * width,
    )
    other = swapped(mine, "c")
    right = jnp.where(core == 0, other, mine).reshape(B, ng, B)
    z = jnp.einsum(
        "zgrk,cgk->zrc", cross_rows, right, precision=lax.Precision.HIGHEST, preferred_element_type=F32
    )
    near = [z, swapped(z, "yl"), swapped(z, "zl"), swapped(z, ("zl", "yl"))]
    came = swapped(jnp.stack(near), "c")
    at = jnp.stack([core, zl, yl]).astype(jnp.int32)
    (out,) = call(
        last_kernel, [at], [mine, other, *near, came], [(rows, B)],
        [pltpu.VMEM((2, nz, 2, 2, rows, B), F32)],
    )
    return out


def solution(mesh):
    torus = Mesh(mesh.devices.reshape(4, 2, 2, 2, 4, 2), AXES)
    return jax.shard_map(
        program,
        mesh=torus,
        in_specs=(P(AXES, None), P(AXES, None), P()),
        out_specs=P(DP, GRP),
        check_vma=False,
    )
```

```python
import functools
import math

import jax
import jax.numpy as jnp
from jax import lax
from jax.experimental import pallas as pl
from jax.experimental.pallas import tpu as pltpu
from jax.sharding import Mesh
from jax.sharding import PartitionSpec as P

INTERPRET = False
STEPS = 14
AXES = ("zh", "zl", "yl", "c", "x", "yh")
DP = ("zh", "zl", "yl", "c")
GRP = ("x", "yh")
Y = ("yl", "yh")
B = 128
F32 = jnp.float32
BF16 = jnp.bfloat16


def sub_segments(start, size, piece):
    done = 0
    while done < size:
        q, r = divmod(start + done, piece)
        n = min(piece - r, size - done)
        yield q, r, done, n
        done += n


def dot(a, b):
    return jnp.dot(a, b, preferred_element_type=F32)


def gram_kernel(nb, colour, core_ref, acts_ref, grads_ref, keep_ref, send_ref, t_ref):
    core = core_ref[0]
    part = nb * (nb + 1) // 2 * B // 2
    piece = part // 16
    strip = nb * B // 4
    rows = (keep_ref.shape[2] - piece) // 4
    acts = acts_ref[...]
    grads = grads_ref[...]
    t_ref[0] = acts.T
    t_ref[1] = grads.T
    for which, out in ((0, send_ref), (1, keep_ref)):
        slot = core if which else 1 - core
        right = jnp.where(slot == 0, acts, grads)
        for jj in range(nb // 2):
            spans = []
            for j in (2 * jj, 2 * jj + 1):
                base = j * (j + 1) // 2 * B
                lo, hi = max(base, colour * part), min(base + (j + 1) * B, (colour + 1) * part)
                if lo < hi:
                    spans.append((j, lo, hi, lo - base, hi - base))
            if not spans:
                continue
            low, high = min(s[3] for s in spans), max(s[4] for s in spans)
            res = dot(t_ref[slot, low:high, :], right[:, jj * 2 * B : (jj + 1) * 2 * B])
            for j, lo, hi, first, _ in spans:
                lane = (j - 2 * jj) * B
                for q, r, at, n in sub_segments(lo - colour * part, hi - lo, piece):
                    at = first - low + at
                    out[q // 4, q % 4, r : r + n, :] = res[at : at + n, lane : lane + B]
        begin = pl.multiple_of(slot * 2 * strip + colour * strip, strip)
        left = t_ref[0, pl.ds(begin, strip), :]
        for x in range(nb // 2):
            res = dot(left, grads[:, x * 2 * B : (x + 1) * 2 * B])
            for s in range(strip // rows):
                zh, yl = divmod(s, 2)
                for yh in range(2):
                    y = yh * 2 + yl
                    first, second = (y, x) if colour else (x, y)
                    at = piece + zh * rows
                    out[first, second, at : at + rows, :] = res[s * rows : s * rows + rows, yh * B : yh * B + B]


def turned_kernel(count, at_ref, *refs):
    ins, outs = refs[:count], refs[count:]
    for k, out in enumerate(outs):
        z = lax.rem(at_ref[0] + k, len(outs))
        total = ins[0][z]
        for ref in ins[1:]:
            total = total + ref[z]
        out[...] = total


def halves_kernel(at_ref, *refs):
    count = (len(refs) - 2) // 2
    sums = []
    for refs_of in (refs[:count], refs[count : 2 * count]):
        total = refs_of[0][...]
        for ref in refs_of[1:]:
            total = total + ref[...]
        sums.append(total)
    keep_ref, send_ref = refs[-2:]
    low = at_ref[0] == 0
    keep_ref[...] = jnp.where(low, sums[0], sums[1])
    send_ref[...] = jnp.where(low, sums[1], sums[0])


def ring_kernel(piece, at_ref, keep_ref, came_ref, *refs):
    outs, sum_ref = refs[:-1], refs[-1]
    sum_ref[...] = keep_ref[...] + came_ref[...]
    rows = outs[0].shape[0] - piece
    for k, out in enumerate(outs):
        z = lax.rem(at_ref[0] + k, len(outs))
        out[:piece, :] = sum_ref[:piece, :]
        out[piece:, :] = sum_ref[pl.ds(pl.multiple_of(piece + z * rows, 8), rows), :]


def total_kernel(scale, *refs):
    factor_ref, cross_ref = refs[-2:]
    total = refs[0][...]
    for ref in refs[1:-2]:
        total = total + ref[...]
    piece = factor_ref.shape[0]
    factor_ref[...] = total[:piece]
    cross_ref[...] = total[piece:] * scale


def colours_kernel(at_ref, mine_ref, other_ref, *outs):
    mine, other = mine_ref[...], other_ref[...]
    low = at_ref[0] == 0
    outs[0][...] = jnp.where(low, mine, other)
    outs[1][...] = jnp.where(low, other, mine)


def joined_kernel(*refs):
    outs = refs[-3:]
    count = (len(refs) - 4) // 2
    for k in range(count):
        outs[0][k] = refs[k][...]
        outs[1][k] = refs[count + k][...]
    cross = refs[2 * count][...]
    for q in range(outs[2].shape[0]):
        outs[2][q] = cross


def last_kernel(at_ref, mine_ref, other_ref, *refs):
    out_ref, z_ref = refs[-2:]
    core, zl, yl = at_ref[0], at_ref[1], at_ref[2]
    own, came = refs[:4], refs[4]
    for d in range(4):
        dz, dy = divmod(d, 2)
        pz, py = jnp.bitwise_xor(zl, dz), jnp.bitwise_xor(yl, dy)
        for zh in range(z_ref.shape[2]):
            z_ref[core, pz, zh, py] = own[d][zh]
            z_ref[1 - core, pz, zh, py] = came[d, zh]
    rows = out_ref.shape[0]
    first = pl.multiple_of(yl * 2 * rows + core * rows, 8)
    mine = mine_ref[pl.ds(first, rows), :]
    other = other_ref[pl.ds(first, rows), :]
    hi, lo = split(jnp.where(core == 0, mine, other))
    zhi, zlo = split(z_ref[...].reshape(-1, B))
    out_ref[...] = (dot(hi, zlo) + dot(lo, zhi)) + dot(hi, zhi)


def split(v):
    hi = v.astype(BF16)
    return hi, (v - hi.astype(F32)).astype(BF16)


def inverse_kernel(nb, scale, at_ref, damp_ref, *refs):
    out_ref, p_ref, m_ref, hi_ref, lo_ref, s_ref, y_ref = refs[-7:]
    width = nb * B
    damp = damp_ref[0]
    for colour in range(2):
        first, second = at_ref[1 + colour], at_ref[2 - colour]
        for k in range(4):
            for i in range(4):
                p = colour * 16 + lax.rem(first + 4 - k, 4) * 4 + lax.rem(second + 4 - i, 4)
                p_ref[p] = refs[colour * 4 + k][i]
    eye = (lax.broadcasted_iota(jnp.int32, (B, B), 0) == lax.broadcasted_iota(jnp.int32, (B, B), 1)).astype(F32)
    for j in range(nb):
        base = j * (j + 1) // 2 * B
        for i in range(j + 1):
            parts = []
            for q, r, _, n in sub_segments(base + i * B, B, p_ref.shape[1]):
                parts.append(p_ref[q, r : r + n, :])
            block = jnp.concatenate(parts, axis=0) * scale
            if i == j:
                block = block + damp * eye
            m_ref[i * B : (i + 1) * B, j * B : (j + 1) * B] = block
            if i != j:
                m_ref[j * B : (j + 1) * B, i * B : (i + 1) * B] = block.T
    total = jnp.zeros((8, width), F32)
    for i in range(nb):
        total = total + jnp.abs(m_ref[i * B : (i + 1) * B, :]).reshape(B // 8, 8, width).sum(axis=0)
    alpha = 1.0 / jnp.max(jnp.sum(total, axis=0, keepdims=True), axis=1, keepdims=True)
    for i in range(nb):
        rows = lax.broadcasted_iota(jnp.int32, (B, width), 0) + i * B
        ones = (rows == lax.broadcasted_iota(jnp.int32, (B, width), 1)).astype(F32)
        hi, lo = split(ones - alpha * m_ref[i * B : (i + 1) * B, :])
        hi_ref[i * B : (i + 1) * B, :] = hi
        lo_ref[i * B : (i + 1) * B, :] = lo
    start = pl.multiple_of(at_ref[0], B)
    rows = lax.broadcasted_iota(jnp.int32, (B, width), 0) + start
    ones = (rows == lax.broadcasted_iota(jnp.int32, (B, width), 1)).astype(F32)
    s_ref[...] = ones
    y_ref[...] = 2.0 * ones - alpha * m_ref[pl.ds(start, B), :]

    def step(_, carry):
        hi, lo = split(y_ref[...])
        both = jnp.concatenate([hi, lo], axis=0)
        first = dot(both, hi_ref[...])
        y_ref[...] = (dot(hi, lo_ref[...]) + first[B:]) + first[:B] + s_ref[...]
        return carry

    lax.fori_loop(0, STEPS, step, 0)
    out_ref[...] = alpha * y_ref[...]


def vmem(n):
    return [pl.BlockSpec(memory_space=pltpu.VMEM)] * n


def smem(n=1):
    return [pl.BlockSpec(memory_space=pltpu.SMEM)] * n


def call(kernel, scalars, arrays, outs, scratch=(), flops=0, limit=32):
    moved = sum(4 * math.prod(o) for o in outs) + sum(a.size * a.dtype.itemsize for a in arrays)
    shapes = [jax.ShapeDtypeStruct(o, F32) for o in outs]
    return pl.pallas_call(
        kernel,
        out_shape=shapes,
        in_specs=smem(len(scalars)) + vmem(len(arrays)),
        out_specs=vmem(len(outs)),
        scratch_shapes=list(scratch),
        cost_estimate=pl.CostEstimate(flops=flops, bytes_accessed=moved, transcendentals=0),
        compiler_params=pltpu.CompilerParams(vmem_limit_bytes=limit << 20),
        interpret=INTERPRET,
    )(*[jnp.atleast_1d(s) for s in scalars], *arrays)


def swapped(array, axes):
    pairs = [(k, lax.axis_size(axes) - 1 - k) for k in range(lax.axis_size(axes))]
    return lax.ppermute(array, axes, pairs)


def shifted(array, axis, by):
    size = lax.axis_size(axis)
    spots = [k % 2 * 2 + k // 2 for k in range(4)] if axis == Y else list(range(size))
    return lax.ppermute(array, axis, [(spots[k], spots[(k + by) % size]) for k in range(size)])


def program(acts, grads, damping):
    tokens, width = acts.shape
    nb = width // B
    ng, nz = lax.axis_size(GRP), lax.axis_size("zh")
    scale = 1.0 / (tokens * lax.axis_size(AXES))
    core, zh, zl, yl, x, yh = (lax.axis_index(a) for a in ("c", "zh", "zl", "yl", "x", "yh"))
    y = yh * 2 + yl
    rings = (("x", x), (Y, y))
    piece = nb * (nb + 1) // 2 * B // 32
    rows = width // lax.axis_size(DP)
    chunk = (piece + nz * rows, B)

    near = []
    for colour in range(2):
        kept, sent = call(
            functools.partial(gram_kernel, nb, colour), [core], [acts, grads],
            [(4, 4, *chunk)] * 2, [pltpu.VMEM((2, width, tokens), BF16)], flops=2 * tokens * width * width,
        )
        near.append([kept, swapped(sent, "c")])
    for depth in range(2):
        far = []
        for colour in range(2):
            ring, at = rings[depth ^ colour]
            shape = chunk if depth else (4, *chunk)
            turned = call(
                functools.partial(turned_kernel, len(near[colour])), [at], near[colour],
                [shape] * 4,
            )
            far.append([turned[0]] + [shifted(turned[k], ring, k) for k in (2, 1, 3)])
        near = far
    keep, send = call(halves_kernel, [zl], near[0] + near[1], [chunk] * 2)
    turned = call(
        functools.partial(ring_kernel, piece), [zh], [keep, swapped(send, "zl")],
        [(piece + rows, B)] * nz, [pltpu.VMEM(chunk, F32)],
    )
    around = [turned[0]] + [shifted(turned[k], "zh", k) for k in (2, 1, 3)]
    mine, cross = call(functools.partial(total_kernel, scale), [], around, [(piece, B), (rows, B)])
    stretches = call(colours_kernel, [zl], [mine, swapped(mine, "zl")], [(piece, B)] * 2)
    parts = []
    for colour in range(2):
        ring = rings[1 - colour][0]
        parts += [stretches[colour]] + [shifted(stretches[colour], ring, k) for k in (1, 2, 3)]
    spread = ("zh", "x", "yh")
    *joined, crosses = call(
        joined_kernel, [], [*parts, cross],
        [(4, piece, B), (4, piece, B), (lax.axis_size(spread), rows, B)],
    )
    pieces = []
    for colour in range(2):
        ring = rings[colour][0]
        moved = {k: shifted(joined[colour], ring, k) for k in (2, 1, 3)}
        pieces += [joined[colour]] + [moved[k] for k in (1, 2, 3)]
    cross_rows = lax.all_to_all(crosses, spread, 0, 0, tiled=True).reshape(nz, ng, rows, B)
    height = zh * lax.axis_size("zl") + zl
    start = jnp.where(core == 0, height * B, lax.axis_index(GRP) * B).astype(jnp.int32)
    damp = jnp.where(core == 0, damping[0], damping[1])
    (mine,) = call(
        functools.partial(inverse_kernel, nb, scale), [jnp.stack([start, x, y]), damp], pieces,
        [(B, width)],
        [
            pltpu.VMEM((32, piece, B), F32),
            pltpu.VMEM((width, width), F32),
            pltpu.VMEM((width, width), BF16),
            pltpu.VMEM((width, width), BF16),
            pltpu.VMEM((B, width), F32),
            pltpu.VMEM((B, width), F32),
        ],
        flops=2 * 3 * STEPS * B * width * width,
    )
    other = swapped(mine, "c")
    right = jnp.where(core == 0, other, mine).reshape(B, ng, B)
    z = jnp.einsum(
        "zgrk,cgk->zrc", cross_rows, right, precision=lax.Precision.HIGHEST, preferred_element_type=F32
    )
    slabs = [z, swapped(z, "yl"), swapped(z, "zl"), swapped(z, ("zl", "yl"))]
    came = swapped(jnp.stack(slabs), "c")
    (out,) = call(
        last_kernel, [jnp.stack([core, zl, yl])], [mine, other, *slabs, came], [(rows, B)],
        [pltpu.VMEM((2, 2, nz, 2, rows, B), F32)],
    )
    return out


def solution(mesh):
    torus = Mesh(mesh.devices.reshape(4, 2, 2, 2, 4, 2), AXES)
    return jax.shard_map(
        program,
        mesh=torus,
        in_specs=(P(AXES, None), P(AXES, None), P()),
        out_specs=P(DP, GRP),
        check_vma=False,
    )
```

```python
import functools
import math

import jax
import jax.numpy as jnp
from jax import lax
from jax.experimental import pallas as pl
from jax.experimental.pallas import tpu as pltpu
from jax.sharding import Mesh
from jax.sharding import PartitionSpec as P


INTERPRET = False
STEPS = 14
AXES = ("zh", "zl", "yl", "c", "x", "yh")
ZH, ZL, YL, CORE, X, YH = range(6)
DP = ("zh", "zl", "yl", "c")
GRP = ("x", "yh")
Y = ("yl", "yh")
PLANE = ("zl", "yl", "x", "yh")
B = 128
F32 = jnp.float32
BF16 = jnp.bfloat16


def ring_places(at_ref):
    return at_ref[X], at_ref[YH] * 2 + at_ref[YL]


def sub_segments(start, size, piece):
    done = 0
    while done < size:
        q, r = divmod(start + done, piece)
        n = min(piece - r, size - done)
        yield q, r, done, n
        done += n


def dot(a, b):
    return jnp.dot(a, b, preferred_element_type=F32)


def gram_terms(nb, colour, which, core, acts_ref, grads_ref, t_ref, out):
    part = nb * (nb + 1) // 2 * B // 2
    piece = part // 16
    strip = nb * B // 4
    rows = (out.shape[2] - piece) // 4
    grads = grads_ref[...]
    slot = core if which else 1 - core
    right = jnp.where(slot == 0, acts_ref[...], grads)
    for jj in range(nb // 2):
        spans = []
        for j in (2 * jj, 2 * jj + 1):
            base = j * (j + 1) // 2 * B
            lo, hi = max(base, colour * part), min(base + (j + 1) * B, (colour + 1) * part)
            if lo < hi:
                spans.append((j, lo, hi, lo - base, hi - base))
        if not spans:
            continue
        low, high = min(s[3] for s in spans), max(s[4] for s in spans)
        res = dot(t_ref[slot, low:high, :], right[:, jj * 2 * B : (jj + 1) * 2 * B])
        for j, lo, hi, first, _ in spans:
            lane = (j - 2 * jj) * B
            for q, r, at, n in sub_segments(lo - colour * part, hi - lo, piece):
                at = first - low + at
                out[q // 4, q % 4, r : r + n, :] = res[at : at + n, lane : lane + B]
    begin = pl.multiple_of(slot * 2 * strip + colour * strip, strip)
    left = t_ref[0, pl.ds(begin, strip), :]
    for x in range(nb // 2):
        res = dot(left, grads[:, x * 2 * B : (x + 1) * 2 * B])
        for s in range(strip // rows):
            zh, yl = divmod(s, 2)
            for yh in range(2):
                y = yh * 2 + yl
                first, second = (y, x) if colour else (x, y)
                at = piece + zh * rows
                out[first, second, at : at + rows, :] = res[s * rows : s * rows + rows, yh * B : yh * B + B]


def gram_kernel(nb, colour, which, at_ref, acts_ref, grads_ref, t_ref, out_ref):
    gram_terms(nb, colour, which, at_ref[CORE], acts_ref, grads_ref, t_ref, out_ref)


def first_kernel(nb, colour, at_ref, acts_ref, grads_ref, t_ref, out_ref):
    t_ref[0] = acts_ref[...].T
    t_ref[1] = grads_ref[...].T
    gram_terms(nb, colour, 0, at_ref[CORE], acts_ref, grads_ref, t_ref, out_ref)


def turned_kernel(count, colour, at_ref, *refs):
    ins, outs = refs[:count], refs[count:]
    for k, out in enumerate(outs):
        z = lax.rem(ring_places(at_ref)[colour] + k, len(outs))
        total = ins[0][z]
        for ref in ins[1:]:
            total = total + ref[z]
        out[...] = total


def sorted_kernel(at_ref, *refs):
    ins, outs = refs[:8], refs[8:]
    low = at_ref[ZL] == 0
    x, y = ring_places(at_ref)
    for k in range(4):
        sums = []
        for colour in range(2):
            z = lax.rem((y, x)[colour] + k, 4)
            total = ins[colour * 4][z]
            for ref in ins[colour * 4 + 1 : colour * 4 + 4]:
                total = total + ref[z]
            sums.append(total)
        outs[k][...] = jnp.where(low, sums[0], sums[1])
        outs[4 + k][...] = jnp.where(low, sums[1], sums[0])


def ring_kernel(piece, at_ref, *refs):
    ins, outs, sum_ref = refs[:8], refs[8:-1], refs[-1]
    total = ins[0][...]
    for ref in ins[1:]:
        total = total + ref[...]
    sum_ref[...] = total
    rows = outs[0].shape[0] - piece
    for k, out in enumerate(outs):
        z = lax.rem(at_ref[ZH] + k, len(outs))
        out[:piece, :] = sum_ref[:piece, :]
        out[piece:, :] = sum_ref[pl.ds(pl.multiple_of(piece + z * rows, 8), rows), :]


def total_kernel(scale, at_ref, *refs):
    factor_ref, cross_ref = refs[-2:]
    total = refs[0][...]
    for ref in refs[1:-2]:
        total = total + ref[...]
    piece = factor_ref.shape[0]
    factor_ref[...] = total[:piece]
    cross_ref[...] = total[piece:] * scale


def joined_kernel(at_ref, *refs):
    outs = refs[-3:]
    low = at_ref[ZL] == 0
    for k in range(4):
        own, other = refs[k][...], refs[4 + k][...]
        outs[0][k] = jnp.where(low, own, other)
        outs[1][k] = jnp.where(low, other, own)
    cross = refs[8][...]
    for q in range(outs[2].shape[0]):
        outs[2][q] = cross


def rows_kernel(at_ref, cross_ref, mine_ref, other_ref, out_ref, c_ref):
    count, rows, _ = cross_ref.shape
    groups = c_ref.shape[1] // B
    for k in range(count):
        zh, g = divmod(k, groups)
        c_ref[zh * rows : zh * rows + rows, g * B : g * B + B] = cross_ref[k]
    hi, lo = split(c_ref[...])
    rhi, rlo = split(jnp.where(at_ref[CORE] == 0, other_ref[...], mine_ref[...]))
    out_ref[...] = ((dot_t(hi, rlo) + dot_t(lo, rhi)) + dot_t(hi, rhi)).reshape(out_ref.shape)


def last_kernel(at_ref, mine_ref, other_ref, *refs):
    out_ref, z_ref = refs[-2:]
    core, zl, yl = at_ref[CORE], at_ref[ZL], at_ref[YL]
    own, came = refs[:4], refs[4]
    for d in range(4):
        dz, dy = divmod(d, 2)
        pz, py = jnp.bitwise_xor(zl, dz), jnp.bitwise_xor(yl, dy)
        for zh in range(z_ref.shape[2]):
            z_ref[core, pz, zh, py] = own[d][zh]
            z_ref[1 - core, pz, zh, py] = came[d, zh]
    rows = out_ref.shape[0]
    first = pl.multiple_of(yl * 2 * rows + core * rows, 8)
    mine = mine_ref[pl.ds(first, rows), :]
    other = other_ref[pl.ds(first, rows), :]
    hi, lo = split(jnp.where(core == 0, mine, other))
    zhi, zlo = split(z_ref[...].reshape(-1, B))
    out_ref[...] = (dot(hi, zlo) + dot(lo, zhi)) + dot(hi, zhi)


def dot_t(a, b):
    return lax.dot_general(a, b, (((1,), (1,)), ((), ())), preferred_element_type=F32)


def split(v):
    hi = v.astype(BF16)
    return hi, (v - hi.astype(F32)).astype(BF16)


def inverse_kernel(nb, scale, at_ref, damp_ref, *refs):
    out_ref, p_ref, m_ref, hi_ref, lo_ref, s_ref, y_ref = refs[-7:]
    width = nb * B
    core = at_ref[CORE]
    damp = jnp.where(core == 0, damp_ref[0], damp_ref[1])
    places = ring_places(at_ref)
    for colour in range(2):
        first, second = places[colour], places[1 - colour]
        for k in range(4):
            for i in range(4):
                p = colour * 16 + lax.rem(first + 4 - k, 4) * 4 + lax.rem(second + 4 - i, 4)
                p_ref[p] = refs[colour * 4 + k][i]
    eye = (lax.broadcasted_iota(jnp.int32, (B, B), 0) == lax.broadcasted_iota(jnp.int32, (B, B), 1)).astype(F32)
    for j in range(nb):
        base = j * (j + 1) // 2 * B
        for i in range(j + 1):
            parts = []
            for q, r, _, n in sub_segments(base + i * B, B, p_ref.shape[1]):
                parts.append(p_ref[q, r : r + n, :])
            block = jnp.concatenate(parts, axis=0) * scale
            if i == j:
                block = block + damp * eye
            m_ref[i * B : (i + 1) * B, j * B : (j + 1) * B] = block
            if i != j:
                m_ref[j * B : (j + 1) * B, i * B : (i + 1) * B] = block.T
    total = jnp.zeros((8, width), F32)
    for i in range(nb):
        total = total + jnp.abs(m_ref[i * B : (i + 1) * B, :]).reshape(B // 8, 8, width).sum(axis=0)
    alpha = 1.0 / jnp.max(jnp.sum(total, axis=0, keepdims=True), axis=1, keepdims=True)
    for i in range(nb):
        rows = lax.broadcasted_iota(jnp.int32, (B, width), 0) + i * B
        ones = (rows == lax.broadcasted_iota(jnp.int32, (B, width), 1)).astype(F32)
        hi, lo = split(ones - alpha * m_ref[i * B : (i + 1) * B, :])
        hi_ref[i * B : (i + 1) * B, :] = hi
        lo_ref[i * B : (i + 1) * B, :] = lo
    height = at_ref[ZH] * 2 + at_ref[ZL]
    side = at_ref[X] * 2 + at_ref[YH]
    start = pl.multiple_of(jnp.where(core == 0, height, side) * B, B)
    rows = lax.broadcasted_iota(jnp.int32, (B, width), 0) + start
    ones = (rows == lax.broadcasted_iota(jnp.int32, (B, width), 1)).astype(F32)
    s_ref[...] = ones
    y_ref[...] = 2.0 * ones - alpha * m_ref[pl.ds(start, B), :]

    def step(_, carry):
        hi, lo = split(y_ref[...])
        both = jnp.concatenate([hi, lo], axis=0)
        first = dot(both, hi_ref[...])
        y_ref[...] = (dot(hi, lo_ref[...]) + first[B:]) + first[:B] + s_ref[...]
        return carry

    lax.fori_loop(0, STEPS, step, 0)
    out_ref[...] = alpha * y_ref[...]


def vmem(n):
    return [pl.BlockSpec(memory_space=pltpu.VMEM)] * n


def smem(n=1):
    return [pl.BlockSpec(memory_space=pltpu.SMEM)] * n


def call(kernel, scalars, arrays, outs, scratch=(), flops=0, limit=20):
    shapes = [o if hasattr(o, "dtype") else jax.ShapeDtypeStruct(o, F32) for o in outs]
    moved = sum(math.prod(a.shape) * a.dtype.itemsize for a in [*arrays, *shapes])
    return pl.pallas_call(
        kernel,
        out_shape=shapes,
        in_specs=smem(len(scalars)) + vmem(len(arrays)),
        out_specs=vmem(len(outs)),
        scratch_shapes=list(scratch),
        cost_estimate=pl.CostEstimate(flops=flops, bytes_accessed=moved, transcendentals=0),
        compiler_params=pltpu.CompilerParams(vmem_limit_bytes=limit << 20),
        interpret=INTERPRET,
    )(*scalars, *arrays)


def swapped(array, axes):
    pairs = [(k, lax.axis_size(axes) - 1 - k) for k in range(lax.axis_size(axes))]
    return lax.ppermute(array, axes, pairs)


def shifted(array, axis, by):
    size = lax.axis_size(axis)
    spots = [k % 2 * 2 + k // 2 for k in range(4)] if axis == Y else list(range(size))
    return lax.ppermute(array, axis, [(spots[k], spots[(k + by) % size]) for k in range(size)])


def sent_across(array, by, flip, along_y):
    def place(zl, x, y):
        return ((zl * 2 + y % 2) * 4 + x) * 2 + y // 2

    pairs = []
    for zl in range(2):
        for x in range(4):
            for y in range(4):
                target = (x, (y + by) % 4) if zl == along_y else ((x + by) % 4, y)
                pairs.append((place(zl, x, y), place(zl ^ flip, *target)))
    return lax.ppermute(array, PLANE, pairs)


def program(acts, grads, damping):
    tokens, width = acts.shape
    nb = width // B
    nz = lax.axis_size("zh")
    scale = 1.0 / (tokens * lax.axis_size(AXES))
    bits = [lax.axis_size(a).bit_length() - 1 for a in AXES]
    shifts = jnp.array([sum(bits[k + 1 :]) for k in range(len(bits))], jnp.int32)
    masks = jnp.array([(1 << b) - 1 for b in bits], jnp.int32)
    at = (lax.axis_index(AXES) >> shifts) & masks
    rings = ("x", Y)
    piece = nb * (nb + 1) // 2 * B // 32
    rows = width // lax.axis_size(DP)
    chunk = (piece + nz * rows, B)

    terms = (4, 4, *chunk)
    gram_flops = tokens * width * width
    transposed, sent1 = call(
        functools.partial(first_kernel, nb, 1), [at], [acts, grads],
        [jax.ShapeDtypeStruct((2, width, tokens), BF16), terms], flops=gram_flops,
    )

    def grams(colour, which):
        kernel = functools.partial(gram_kernel, nb, colour, which)
        return call(kernel, [at], [acts, grads, transposed], [terms], flops=gram_flops)[0]

    sent0 = grams(0, 0)
    came = []
    for sent in (sent0, sent1):
        came.append(swapped(sent, "c"))
    far = []
    for colour in (0, 1):
        ring = rings[colour]
        kept = grams(colour, 1)
        turned = call(functools.partial(turned_kernel, 2, colour), [at], [kept, came[colour]], [(4, *chunk)] * 4)
        far += [turned[0]] + [shifted(turned[k], ring, k) for k in (2, 1, 3)]
    sides = call(sorted_kernel, [at], far, [chunk] * 8)
    summands = [sides[0]]
    summands += [sent_across(sides[4 + k], k, 1, 1) for k in (2, 1, 3, 0)]
    summands += [sent_across(sides[k], k, 0, 0) for k in (2, 1, 3)]
    turned = call(
        functools.partial(ring_kernel, piece), [at], summands, [(piece + rows, B)] * nz,
        [pltpu.VMEM(chunk, F32)],
    )
    around = [turned[0]] + [shifted(turned[k], "zh", k) for k in (2, 1, 3)]
    mine, cross = call(functools.partial(total_kernel, scale), [at], around, [(piece, B), (rows, B)])
    other = {k: sent_across(mine, k, 1, 0) for k in (2, 1, 3, 0)}
    same = {k: sent_across(mine, k, 0, 0) for k in (2, 1, 3)}
    spread = ("zh", "x", "yh")
    *joined, crosses = call(
        joined_kernel, [at], [mine, *(same[k] for k in (1, 2, 3)), *(other[k] for k in range(4)), cross],
        [(4, piece, B), (4, piece, B), (lax.axis_size(spread), rows, B)],
    )
    pieces = []
    for colour in range(2):
        ring = rings[colour]
        moved = {k: shifted(joined[colour], ring, k) for k in (2, 1, 3)}
        pieces += [joined[colour]] + [moved[k] for k in (1, 2, 3)]
    cross_rows = lax.all_to_all(crosses, spread, 0, 0, tiled=True)
    (mine,) = call(
        functools.partial(inverse_kernel, nb, scale), [at, damping], pieces,
        [(B, width)],
        [
            pltpu.VMEM((32, piece, B), F32),
            pltpu.VMEM((width, width), F32),
            pltpu.VMEM((width, width), BF16),
            pltpu.VMEM((width, width), BF16),
            pltpu.VMEM((B, width), F32),
            pltpu.VMEM((B, width), F32),
        ],
        flops=2 * 3 * STEPS * B * width * width,
        limit=24,
    )
    other = swapped(mine, "c")
    (z,) = call(rows_kernel, [at], [cross_rows, mine, other], [(nz, rows, B)], [pltpu.VMEM((nz * rows, width), F32)])
    slabs = [z, swapped(z, "yl"), swapped(z, "zl"), swapped(z, ("zl", "yl"))]
    came = swapped(jnp.stack(slabs), "c")
    (out,) = call(
        last_kernel, [at], [mine, other, *slabs, came], [(rows, B)],
        [pltpu.VMEM((2, 2, nz, 2, rows, B), F32)],
    )
    return out


def solution(mesh):
    torus = Mesh(mesh.devices.reshape(4, 2, 2, 2, 4, 2), AXES)
    return jax.shard_map(
        program,
        mesh=torus,
        in_specs=(P(AXES, None), P(AXES, None), P()),
        out_specs=P(DP, GRP),
        check_vma=False,
    )
```

```python
import functools
import math

import jax
import jax.numpy as jnp
from jax import lax
from jax.experimental import pallas as pl
from jax.experimental.pallas import tpu as pltpu
from jax.sharding import Mesh
from jax.sharding import PartitionSpec as P


INTERPRET = False
STEPS = 14
AXES = ("zh", "zl", "yl", "c", "x", "yh")
ZH, ZL, YL, CORE, X, YH = range(6)
DP = ("zh", "zl", "yl", "c")
GRP = ("x", "yh")
Y = ("yl", "yh")
PLANE = ("zl", "yl", "x", "yh")
B = 128
F32 = jnp.float32
BF16 = jnp.bfloat16


def ring_places(at_ref):
    return at_ref[X], at_ref[YH] * 2 + at_ref[YL]


def sub_segments(start, size, piece):
    done = 0
    while done < size:
        q, r = divmod(start + done, piece)
        n = min(piece - r, size - done)
        yield q, r, done, n
        done += n


def dot(a, b):
    return jnp.dot(a, b, preferred_element_type=F32)


def factor_terms(nb, colour, which, core, acts_ref, grads_ref, t_ref, out):
    part = nb * (nb + 1) // 2 * B // 2
    piece = out.shape[2]
    slot = core if which else 1 - core
    right = jnp.where(slot == 0, acts_ref[...], grads_ref[...])
    for jj in range(nb // 2):
        spans = []
        for j in (2 * jj, 2 * jj + 1):
            base = j * (j + 1) // 2 * B
            lo, hi = max(base, colour * part), min(base + (j + 1) * B, (colour + 1) * part)
            if lo < hi:
                spans.append((j, lo, hi, lo - base, hi - base))
        if not spans:
            continue
        low, high = min(s[3] for s in spans), max(s[4] for s in spans)
        res = dot(t_ref[slot, low:high, :], right[:, jj * 2 * B : (jj + 1) * 2 * B])
        for j, lo, hi, first, _ in spans:
            lane = (j - 2 * jj) * B
            for q, r, at, n in sub_segments(lo - colour * part, hi - lo, piece):
                at = first - low + at
                out[q // 4, q % 4, r : r + n, :] = res[at : at + n, lane : lane + B]


def factor_kernel(nb, colour, which, at_ref, acts_ref, grads_ref, t_ref, out_ref):
    factor_terms(nb, colour, which, at_ref[CORE], acts_ref, grads_ref, t_ref, out_ref)


def cross_kernel(nb, which, at_ref, grads_ref, t_ref, out):
    core = at_ref[CORE]
    slot = core if which else 1 - core
    half = nb * B // 2
    _, _, nz, rows, _ = out.shape
    left = t_ref[0, pl.ds(pl.multiple_of(slot * half, half), half), :]
    for x in range(nb // 2):
        res = dot(left, grads_ref[:, x * 2 * B : (x + 1) * 2 * B])
        for s in range(half // rows):
            zl, rest = divmod(s, nz * 2)
            zh, yl = divmod(rest, 2)
            for yh in range(2):
                block = res[s * rows : s * rows + rows, yh * B : yh * B + B]
                out[zl, (yl * (nb // 2) + x) * 2 + yh, zh, :, :] = block


def first_kernel(nb, colour, at_ref, acts_ref, grads_ref, t_ref, out_ref):
    t_ref[0] = acts_ref[...].T
    t_ref[1] = grads_ref[...].T
    factor_terms(nb, colour, 0, at_ref[CORE], acts_ref, grads_ref, t_ref, out_ref)


def turned_kernel(count, axis, at_ref, *refs):
    ins, outs = refs[:count], refs[count:]
    for k, out in enumerate(outs):
        z = lax.rem(ring_places(at_ref)[axis] + k, len(outs))

        def add(i, out=out, z=z):
            total = ins[0][z, i]
            for ref in ins[1:]:
                total = total + ref[z, i]
            out[i] = total

        if out.ndim == 3:
            pl.loop(0, out.shape[0])(add)
        else:
            total = ins[0][z]
            for ref in ins[1:]:
                total = total + ref[z]
            out[...] = total


def parted_kernel(at_ref, kept_ref, came_ref, keep_ref, send_ref):
    zl = at_ref[ZL]

    @pl.loop(0, keep_ref.shape[0])
    def _(i):
        keep_ref[i] = kept_ref[zl, i] + came_ref[zl, i]
        send_ref[i] = kept_ref[1 - zl, i] + came_ref[1 - zl, i]


def halves_kernel(at_ref, *refs):
    keep_ref, send_ref = refs[-2:]
    sums = []
    for ins in (refs[:4], refs[4:8]):
        total = ins[0][...]
        for ref in ins[1:]:
            total = total + ref[...]
        sums.append(total)
    low = at_ref[ZL] == 0
    keep_ref[...] = jnp.where(low, sums[0], sums[1])
    send_ref[...] = jnp.where(low, sums[1], sums[0])


def plus_kernel(a_ref, b_ref, out_ref):
    @pl.loop(0, out_ref.shape[0])
    def _(i):
        out_ref[i] = a_ref[i] + b_ref[i]


def total_kernel(*refs):
    total = refs[0][...]
    for ref in refs[1:-1]:
        total = total + ref[...]
    refs[-1][...] = total


def summed_kernel(at_ref, pieces_ref, *refs):
    outs, sum_ref = refs[:-1], refs[-1]
    total = pieces_ref[0]
    for q in range(1, pieces_ref.shape[0]):
        total = total + pieces_ref[q]
    sum_ref[...] = total
    for k, out in enumerate(outs):
        out[...] = sum_ref[lax.rem(at_ref[ZH] + k, len(outs))]


def joined_kernel(scale, at_ref, *refs):
    outs = refs[-3:]
    low = at_ref[ZL] == 0
    for k in range(4):
        own, other = refs[k][...], refs[4 + k][...]
        outs[0][k] = jnp.where(low, own, other)
        outs[1][k] = jnp.where(low, other, own)
    cross = refs[8][...]
    for ref in refs[9:-3]:
        cross = cross + ref[...]
    cross = cross * scale
    for q in range(outs[2].shape[0]):
        outs[2][q] = cross


def rows_kernel(at_ref, cross_ref, mine_ref, other_ref, out_ref, c_ref):
    count, rows, _ = cross_ref.shape
    groups = c_ref.shape[1] // B
    for k in range(count):
        zh, g = divmod(k, groups)
        c_ref[zh * rows : zh * rows + rows, g * B : g * B + B] = cross_ref[k]
    hi, lo = split(c_ref[...])
    rhi, rlo = split(jnp.where(at_ref[CORE] == 0, other_ref[...], mine_ref[...]))
    out_ref[...] = ((dot_t(hi, rlo) + dot_t(lo, rhi)) + dot_t(hi, rhi)).reshape(out_ref.shape)


def last_kernel(at_ref, mine_ref, other_ref, *refs):
    out_ref, z_ref = refs[-2:]
    core, zl, yl = at_ref[CORE], at_ref[ZL], at_ref[YL]
    own, came = refs[:4], refs[4]
    for d in range(4):
        dz, dy = divmod(d, 2)
        pz, py = jnp.bitwise_xor(zl, dz), jnp.bitwise_xor(yl, dy)
        for zh in range(z_ref.shape[2]):
            z_ref[core, pz, zh, py] = own[d][zh]
            z_ref[1 - core, pz, zh, py] = came[d, zh]
    rows = out_ref.shape[0]
    first = pl.multiple_of(yl * 2 * rows + core * rows, 8)
    mine = mine_ref[pl.ds(first, rows), :]
    other = other_ref[pl.ds(first, rows), :]
    hi, lo = split(jnp.where(core == 0, mine, other))
    zhi, zlo = split(z_ref[...].reshape(-1, B))
    out_ref[...] = (dot(hi, zlo) + dot(lo, zhi)) + dot(hi, zhi)


def dot_t(a, b):
    return lax.dot_general(a, b, (((1,), (1,)), ((), ())), preferred_element_type=F32)


def split(v):
    hi = v.astype(BF16)
    return hi, (v - hi.astype(F32)).astype(BF16)


def inverse_kernel(nb, scale, at_ref, damp_ref, *refs):
    out_ref, p_ref, m_ref, hi_ref, lo_ref, s_ref, y_ref = refs[-7:]
    width = nb * B
    core = at_ref[CORE]
    damp = jnp.where(core == 0, damp_ref[0], damp_ref[1])
    places = ring_places(at_ref)
    for colour in range(2):
        first, second = places[colour], places[1 - colour]
        for k in range(4):
            for i in range(4):
                p = colour * 16 + lax.rem(first + 4 - k, 4) * 4 + lax.rem(second + 4 - i, 4)
                p_ref[p] = refs[colour * 4 + k][i]
    eye = (lax.broadcasted_iota(jnp.int32, (B, B), 0) == lax.broadcasted_iota(jnp.int32, (B, B), 1)).astype(F32)
    for j in range(nb):
        base = j * (j + 1) // 2 * B
        for i in range(j + 1):
            parts = []
            for q, r, _, n in sub_segments(base + i * B, B, p_ref.shape[1]):
                parts.append(p_ref[q, r : r + n, :])
            block = jnp.concatenate(parts, axis=0) * scale
            if i == j:
                block = block + damp * eye
            m_ref[i * B : (i + 1) * B, j * B : (j + 1) * B] = block
            if i != j:
                m_ref[j * B : (j + 1) * B, i * B : (i + 1) * B] = block.T
    total = jnp.zeros((8, width), F32)
    for i in range(nb):
        total = total + jnp.abs(m_ref[i * B : (i + 1) * B, :]).reshape(B // 8, 8, width).sum(axis=0)
    alpha = 1.0 / jnp.max(jnp.sum(total, axis=0, keepdims=True), axis=1, keepdims=True)
    for i in range(nb):
        rows = lax.broadcasted_iota(jnp.int32, (B, width), 0) + i * B
        ones = (rows == lax.broadcasted_iota(jnp.int32, (B, width), 1)).astype(F32)
        hi, lo = split(ones - alpha * m_ref[i * B : (i + 1) * B, :])
        hi_ref[i * B : (i + 1) * B, :] = hi
        lo_ref[i * B : (i + 1) * B, :] = lo
    height = at_ref[ZH] * 2 + at_ref[ZL]
    side = at_ref[X] * 2 + at_ref[YH]
    start = pl.multiple_of(jnp.where(core == 0, height, side) * B, B)
    rows = lax.broadcasted_iota(jnp.int32, (B, width), 0) + start
    ones = (rows == lax.broadcasted_iota(jnp.int32, (B, width), 1)).astype(F32)
    s_ref[...] = ones
    y_ref[...] = 2.0 * ones - alpha * m_ref[pl.ds(start, B), :]

    def step(_, carry):
        hi, lo = split(y_ref[...])
        both = jnp.concatenate([hi, lo], axis=0)
        first = dot(both, hi_ref[...])
        y_ref[...] = (dot(hi, lo_ref[...]) + first[B:]) + first[:B] + s_ref[...]
        return carry

    lax.fori_loop(0, STEPS, step, 0)
    out_ref[...] = alpha * y_ref[...]


def vmem(n):
    return [pl.BlockSpec(memory_space=pltpu.VMEM)] * n


def smem(n=1):
    return [pl.BlockSpec(memory_space=pltpu.SMEM)] * n


def call(kernel, scalars, arrays, outs, scratch=(), flops=0, limit=20, after=()):
    if after:
        count, inner = len(scalars) + len(arrays), kernel

        def kernel(*refs):
            inner(*refs[:count], *refs[count + len(after) :])

    shapes = [o if hasattr(o, "dtype") else jax.ShapeDtypeStruct(o, F32) for o in outs]
    moved = sum(math.prod(a.shape) * a.dtype.itemsize for a in [*arrays, *shapes])
    return pl.pallas_call(
        kernel,
        out_shape=shapes,
        in_specs=smem(len(scalars)) + vmem(len(arrays)) + [pl.BlockSpec(memory_space=pl.ANY)] * len(after),
        out_specs=vmem(len(outs)),
        scratch_shapes=list(scratch),
        cost_estimate=pl.CostEstimate(flops=flops, bytes_accessed=moved, transcendentals=0),
        compiler_params=pltpu.CompilerParams(vmem_limit_bytes=limit << 20),
        interpret=INTERPRET,
    )(*scalars, *arrays, *after)


def swapped(array, axes):
    pairs = [(k, lax.axis_size(axes) - 1 - k) for k in range(lax.axis_size(axes))]
    return lax.ppermute(array, axes, pairs)


def shifted(array, axis, by):
    size = lax.axis_size(axis)
    spots = [k % 2 * 2 + k // 2 for k in range(4)] if axis == Y else list(range(size))
    return lax.ppermute(array, axis, [(spots[k], spots[(k + by) % size]) for k in range(size)])


def sent_across(array, by, flip, along_y):
    def place(zl, x, y):
        return ((zl * 2 + y % 2) * 4 + x) * 2 + y // 2

    pairs = []
    for zl in range(2):
        for x in range(4):
            for y in range(4):
                target = (x, (y + by) % 4) if zl == along_y else ((x + by) % 4, y)
                pairs.append((place(zl, x, y), place(zl ^ flip, *target)))
    return lax.ppermute(array, PLANE, pairs)


def program(acts, grads, damping):
    tokens, width = acts.shape
    nb = width // B
    nz = lax.axis_size("zh")
    scale = 1.0 / (tokens * lax.axis_size(AXES))
    bits = [lax.axis_size(a).bit_length() - 1 for a in AXES]
    shifts = jnp.array([sum(bits[k + 1 :]) for k in range(len(bits))], jnp.int32)
    masks = jnp.array([(1 << b) - 1 for b in bits], jnp.int32)
    at = (lax.axis_index(AXES) >> shifts) & masks
    rings = ("x", Y)
    piece = nb * (nb + 1) // 2 * B // 32
    rows = width // lax.axis_size(DP)
    chunk = (piece, B)
    gram_flops = tokens * width * width
    transposed, sent1 = call(
        functools.partial(first_kernel, nb, 1), [at], [acts, grads],
        [jax.ShapeDtypeStruct((2, width, tokens), BF16), (4, 4, *chunk)], flops=gram_flops,
    )

    def factors(colour, which):
        kernel = functools.partial(factor_kernel, nb, colour, which)
        arrays = [acts, grads, transposed]
        return call(kernel, [at], arrays, [(4, 4, *chunk)], flops=gram_flops // 2)[0]

    def crosses_of(which, after):
        shape = (2, 16, nz, rows, B)
        kernel = functools.partial(cross_kernel, nb, which)
        return call(kernel, [at], [grads, transposed], [shape], flops=gram_flops, after=after)[0]

    sent0 = factors(0, 0)
    came = []
    for sent in (sent0, sent1):
        came.append(swapped(sent, "c"))
    near = []
    for colour in range(2):
        near.append([factors(colour, 1), came[colour]])
    sent2 = crosses_of(0, [near[0][0], near[1][0]])
    cross_came = swapped(sent2, "c")
    for depth in range(2):
        far = []
        for colour in range(2):
            axis = depth ^ colour
            turned = call(
                functools.partial(turned_kernel, len(near[colour]), axis), [at],
                near[colour], [chunk if depth else (4, *chunk)] * 4,
            )
            far.append([turned[0]] + [shifted(turned[k], rings[axis], k) for k in (2, 1, 3)])
        near = far
        if depth == 0:
            begun = [near[0][0], near[1][0]]
    cross_kept = crosses_of(1, begun)
    cross_keep, cross_send = call(parted_kernel, [at], [cross_kept, cross_came], [(16, nz, rows, B)] * 2)
    cross_came = swapped(cross_send, "zl")
    keep, send = call(halves_kernel, [at], near[0] + near[1], [chunk] * 2)
    arrived = swapped(send, "zl")
    (cross_half,) = call(plus_kernel, [], [cross_keep, cross_came], [(16, nz, rows, B)], after=[send])
    cross_pieces = lax.all_to_all(cross_half, PLANE[1:], 0, 0, tiled=True)
    (half,) = call(total_kernel, [], [keep, arrived], [chunk])
    around = [half] + [shifted(half, "zh", k) for k in (2, 1, 3)]
    (mine,) = call(total_kernel, [], around, [chunk])
    turned = call(summed_kernel, [at], [cross_pieces], [(rows, B)] * nz, [pltpu.VMEM((nz, rows, B), F32)])
    crosses = [turned[0]] + [shifted(turned[k], "zh", k) for k in (2, 1, 3)]
    other = {k: sent_across(mine, k, 1, 0) for k in (2, 1, 3, 0)}
    same = {k: sent_across(mine, k, 0, 0) for k in (2, 1, 3)}
    spread = ("zh", "x", "yh")
    *joined, sent_rows = call(
        functools.partial(joined_kernel, scale), [at],
        [mine, *(same[k] for k in (1, 2, 3)), *(other[k] for k in range(4)), *crosses],
        [(4, piece, B), (4, piece, B), (lax.axis_size(spread), rows, B)],
    )
    pieces = []
    for colour in range(2):
        ring = rings[colour]
        moved = {k: shifted(joined[colour], ring, k) for k in (2, 1, 3)}
        pieces += [joined[colour]] + [moved[k] for k in (1, 2, 3)]
    cross_rows = lax.all_to_all(sent_rows, spread, 0, 0, tiled=True)
    (mine,) = call(
        functools.partial(inverse_kernel, nb, scale), [at, damping], pieces,
        [(B, width)],
        [
            pltpu.VMEM((32, piece, B), F32),
            pltpu.VMEM((width, width), F32),
            pltpu.VMEM((width, width), BF16),
            pltpu.VMEM((width, width), BF16),
            pltpu.VMEM((B, width), F32),
            pltpu.VMEM((B, width), F32),
        ],
        flops=2 * 3 * STEPS * B * width * width,
        limit=24,
    )
    other = swapped(mine, "c")
    (z,) = call(rows_kernel, [at], [cross_rows, mine, other], [(nz, rows, B)], [pltpu.VMEM((nz * rows, width), F32)])
    slabs = [z, swapped(z, "yl"), swapped(z, "zl"), swapped(z, ("zl", "yl"))]
    came = swapped(jnp.stack(slabs), "c")
    (out,) = call(
        last_kernel, [at], [mine, other, *slabs, came], [(rows, B)],
        [pltpu.VMEM((2, 2, nz, 2, rows, B), F32)],
    )
    return out


def solution(mesh):
    torus = Mesh(mesh.devices.reshape(4, 2, 2, 2, 4, 2), AXES)
    return jax.shard_map(
        program,
        mesh=torus,
        in_specs=(P(AXES, None), P(AXES, None), P()),
        out_specs=P(DP, GRP),
        check_vma=False,
    )
```

```python
import functools
import math

import jax
import jax.numpy as jnp
from jax import lax
from jax.experimental import pallas as pl
from jax.experimental.pallas import tpu as pltpu
from jax.sharding import Mesh
from jax.sharding import PartitionSpec as P


INTERPRET = False
STEPS = 14
AXES = ("zh", "zl", "yl", "c", "x", "yh")
ZH, ZL, YL, CORE, X, YH = range(6)
DP = ("zh", "zl", "yl", "c")
GRP = ("x", "yh")
Y = ("yl", "yh")
PLANE = ("zl", "yl", "x", "yh")
B = 128
F32 = jnp.float32
BF16 = jnp.bfloat16


def ring_places(at_ref):
    return at_ref[X], at_ref[YH] * 2 + at_ref[YL]


def sub_segments(start, size, piece):
    done = 0
    while done < size:
        q, r = divmod(start + done, piece)
        n = min(piece - r, size - done)
        yield q, r, done, n
        done += n


def dot(a, b):
    return jnp.dot(a, b, preferred_element_type=F32)


def factor_terms(nb, colour, which, core, acts_ref, grads_ref, t_ref, out):
    part = nb * (nb + 1) // 2 * B // 2
    piece = out.shape[2]
    slot = core if which else 1 - core
    right = jnp.where(slot == 0, acts_ref[...], grads_ref[...])
    for jj in range(nb // 2):
        spans = []
        for j in (2 * jj, 2 * jj + 1):
            base = j * (j + 1) // 2 * B
            lo, hi = max(base, colour * part), min(base + (j + 1) * B, (colour + 1) * part)
            if lo < hi:
                spans.append((j, lo, hi, lo - base, hi - base))
        if not spans:
            continue
        low, high = min(s[3] for s in spans), max(s[4] for s in spans)
        res = dot(t_ref[slot, low:high, :], right[:, jj * 2 * B : (jj + 1) * 2 * B])
        for j, lo, hi, first, _ in spans:
            lane = (j - 2 * jj) * B
            for q, r, at, n in sub_segments(lo - colour * part, hi - lo, piece):
                at = first - low + at
                out[q // 4, q % 4, r : r + n, :] = res[at : at + n, lane : lane + B]


def factor_kernel(nb, colour, which, at_ref, acts_ref, grads_ref, t_ref, out_ref):
    factor_terms(nb, colour, which, at_ref[CORE], acts_ref, grads_ref, t_ref, out_ref)


def cross_kernel(nb, which, at_ref, grads_ref, t_ref, out):
    core = at_ref[CORE]
    slot = core if which else 1 - core
    half = nb * B // 2
    _, _, nz, rows, _ = out.shape
    left = t_ref[0, pl.ds(pl.multiple_of(slot * half, half), half), :]
    for x in range(nb // 2):
        res = dot(left, grads_ref[:, x * 2 * B : (x + 1) * 2 * B])
        for s in range(half // rows):
            zl, rest = divmod(s, nz * 2)
            zh, yl = divmod(rest, 2)
            for yh in range(2):
                block = res[s * rows : s * rows + rows, yh * B : yh * B + B]
                out[zl, (yl * (nb // 2) + x) * 2 + yh, zh, :, :] = block


def first_kernel(nb, colour, at_ref, acts_ref, grads_ref, t_ref, out_ref):
    t_ref[0] = acts_ref[...].T
    t_ref[1] = grads_ref[...].T
    factor_terms(nb, colour, 0, at_ref[CORE], acts_ref, grads_ref, t_ref, out_ref)


def turned_kernel(count, axis, at_ref, *refs):
    ins, outs = refs[:count], refs[count:]
    for k, out in enumerate(outs):
        z = lax.rem(ring_places(at_ref)[axis] + k, len(outs))

        def add(i, out=out, z=z):
            total = ins[0][z, i]
            for ref in ins[1:]:
                total = total + ref[z, i]
            out[i] = total

        if out.ndim == 3:
            pl.loop(0, out.shape[0])(add)
        else:
            total = ins[0][z]
            for ref in ins[1:]:
                total = total + ref[z]
            out[...] = total


def parted_kernel(at_ref, kept_ref, came_ref, keep_ref, send_ref):
    zl = at_ref[ZL]

    @pl.loop(0, keep_ref.shape[0])
    def _(i):
        keep_ref[i] = kept_ref[zl, i] + came_ref[zl, i]
        send_ref[i] = kept_ref[1 - zl, i] + came_ref[1 - zl, i]


def halves_kernel(at_ref, *refs):
    keep_ref, send_ref = refs[-2:]
    sums = []
    for ins in (refs[:4], refs[4:8]):
        total = ins[0][...]
        for ref in ins[1:]:
            total = total + ref[...]
        sums.append(total)
    low = at_ref[ZL] == 0
    keep_ref[...] = jnp.where(low, sums[0], sums[1])
    send_ref[...] = jnp.where(low, sums[1], sums[0])


def plus_kernel(a_ref, b_ref, out_ref):
    @pl.loop(0, out_ref.shape[0])
    def _(i):
        out_ref[i] = a_ref[i] + b_ref[i]


def total_kernel(*refs):
    total = refs[0][...]
    for ref in refs[1:-1]:
        total = total + ref[...]
    refs[-1][...] = total


def summed_kernel(pieces_ref, out_ref):
    total = pieces_ref[0]
    for q in range(1, pieces_ref.shape[0]):
        total = total + pieces_ref[q]
    out_ref[...] = total


def joined_kernel(at_ref, *refs):
    outs = refs[-2:]
    low = at_ref[ZL] == 0
    for k in range(4):
        own, other = refs[k][...], refs[4 + k][...]
        outs[0][k] = jnp.where(low, own, other)
        outs[1][k] = jnp.where(low, other, own)


def repeated_kernel(scale, pieces_ref, out_ref):
    cross = pieces_ref[0]
    for k in range(1, pieces_ref.shape[0]):
        cross = cross + pieces_ref[k]
    cross = cross * scale
    for q in range(out_ref.shape[0]):
        out_ref[q] = cross


def rows_kernel(at_ref, cross_ref, mine_ref, other_ref, out_ref, c_ref):
    count, rows, _ = cross_ref.shape
    groups = c_ref.shape[1] // B
    for k in range(count):
        zh, g = divmod(k, groups)
        c_ref[zh * rows : zh * rows + rows, g * B : g * B + B] = cross_ref[k]
    hi, lo = split(c_ref[...])
    rhi, rlo = split(jnp.where(at_ref[CORE] == 0, other_ref[...], mine_ref[...]))
    out_ref[...] = ((dot_t(hi, rlo) + dot_t(lo, rhi)) + dot_t(hi, rhi)).reshape(out_ref.shape)


def last_kernel(at_ref, mine_ref, other_ref, *refs):
    out_ref, z_ref = refs[-2:]
    core, zl, yl = at_ref[CORE], at_ref[ZL], at_ref[YL]
    own, came = refs[:4], refs[4]
    for d in range(4):
        dz, dy = divmod(d, 2)
        pz, py = jnp.bitwise_xor(zl, dz), jnp.bitwise_xor(yl, dy)
        for zh in range(z_ref.shape[2]):
            z_ref[core, pz, zh, py] = own[d][zh]
            z_ref[1 - core, pz, zh, py] = came[d, zh]
    rows = out_ref.shape[0]
    first = pl.multiple_of(yl * 2 * rows + core * rows, 8)
    mine = mine_ref[pl.ds(first, rows), :]
    other = other_ref[pl.ds(first, rows), :]
    hi, lo = split(jnp.where(core == 0, mine, other))
    zhi, zlo = split(z_ref[...].reshape(-1, B))
    out_ref[...] = (dot(hi, zlo) + dot(lo, zhi)) + dot(hi, zhi)


def dot_t(a, b):
    return lax.dot_general(a, b, (((1,), (1,)), ((), ())), preferred_element_type=F32)


def split(v):
    hi = v.astype(BF16)
    return hi, (v - hi.astype(F32)).astype(BF16)


def inverse_kernel(nb, scale, at_ref, damp_ref, *refs):
    out_ref, p_ref, m_ref, hi_ref, lo_ref, s_ref, y_ref = refs[-7:]
    width = nb * B
    core = at_ref[CORE]
    damp = jnp.where(core == 0, damp_ref[0], damp_ref[1])
    places = ring_places(at_ref)
    for colour in range(2):
        first, second = places[colour], places[1 - colour]
        for k in range(4):
            for i in range(4):
                p = colour * 16 + lax.rem(first + 4 - k, 4) * 4 + lax.rem(second + 4 - i, 4)
                p_ref[p] = refs[colour * 4 + k][i]
    eye = (lax.broadcasted_iota(jnp.int32, (B, B), 0) == lax.broadcasted_iota(jnp.int32, (B, B), 1)).astype(F32)
    for j in range(nb):
        base = j * (j + 1) // 2 * B
        for i in range(j + 1):
            parts = []
            for q, r, _, n in sub_segments(base + i * B, B, p_ref.shape[1]):
                parts.append(p_ref[q, r : r + n, :])
            block = jnp.concatenate(parts, axis=0) * scale
            if i == j:
                block = block + damp * eye
            m_ref[i * B : (i + 1) * B, j * B : (j + 1) * B] = block
            if i != j:
                m_ref[j * B : (j + 1) * B, i * B : (i + 1) * B] = block.T
    total = jnp.zeros((8, width), F32)
    for i in range(nb):
        total = total + jnp.abs(m_ref[i * B : (i + 1) * B, :]).reshape(B // 8, 8, width).sum(axis=0)
    alpha = 1.0 / jnp.max(jnp.sum(total, axis=0, keepdims=True), axis=1, keepdims=True)
    for i in range(nb):
        rows = lax.broadcasted_iota(jnp.int32, (B, width), 0) + i * B
        ones = (rows == lax.broadcasted_iota(jnp.int32, (B, width), 1)).astype(F32)
        hi, lo = split(ones - alpha * m_ref[i * B : (i + 1) * B, :])
        hi_ref[i * B : (i + 1) * B, :] = hi
        lo_ref[i * B : (i + 1) * B, :] = lo
    height = at_ref[ZH] * 2 + at_ref[ZL]
    side = at_ref[X] * 2 + at_ref[YH]
    start = pl.multiple_of(jnp.where(core == 0, height, side) * B, B)
    rows = lax.broadcasted_iota(jnp.int32, (B, width), 0) + start
    ones = (rows == lax.broadcasted_iota(jnp.int32, (B, width), 1)).astype(F32)
    s_ref[...] = ones
    y_ref[...] = 2.0 * ones - alpha * m_ref[pl.ds(start, B), :]

    def step(_, carry):
        hi, lo = split(y_ref[...])
        both = jnp.concatenate([hi, lo], axis=0)
        first = dot(both, hi_ref[...])
        y_ref[...] = (dot(hi, lo_ref[...]) + first[B:]) + first[:B] + s_ref[...]
        return carry

    lax.fori_loop(0, STEPS, step, 0)
    out_ref[...] = alpha * y_ref[...]


def vmem(n):
    return [pl.BlockSpec(memory_space=pltpu.VMEM)] * n


def smem(n=1):
    return [pl.BlockSpec(memory_space=pltpu.SMEM)] * n


def call(kernel, scalars, arrays, outs, scratch=(), flops=0, limit=20, after=()):
    if after:
        count, inner = len(scalars) + len(arrays), kernel

        def kernel(*refs):
            inner(*refs[:count], *refs[count + len(after) :])

    shapes = [o if hasattr(o, "dtype") else jax.ShapeDtypeStruct(o, F32) for o in outs]
    moved = sum(math.prod(a.shape) * a.dtype.itemsize for a in [*arrays, *shapes])
    return pl.pallas_call(
        kernel,
        out_shape=shapes,
        in_specs=smem(len(scalars)) + vmem(len(arrays)) + [pl.BlockSpec(memory_space=pl.ANY)] * len(after),
        out_specs=vmem(len(outs)),
        scratch_shapes=list(scratch),
        cost_estimate=pl.CostEstimate(flops=flops, bytes_accessed=moved, transcendentals=0),
        compiler_params=pltpu.CompilerParams(vmem_limit_bytes=limit << 20),
        interpret=INTERPRET,
    )(*scalars, *arrays, *after)


def swapped(array, axes):
    pairs = [(k, lax.axis_size(axes) - 1 - k) for k in range(lax.axis_size(axes))]
    return lax.ppermute(array, axes, pairs)


def shifted(array, axis, by):
    size = lax.axis_size(axis)
    spots = [k % 2 * 2 + k // 2 for k in range(4)] if axis == Y else list(range(size))
    return lax.ppermute(array, axis, [(spots[k], spots[(k + by) % size]) for k in range(size)])


def sent_across(array, by, flip, along_y):
    def place(zl, x, y):
        return ((zl * 2 + y % 2) * 4 + x) * 2 + y // 2

    pairs = []
    for zl in range(2):
        for x in range(4):
            for y in range(4):
                target = (x, (y + by) % 4) if zl == along_y else ((x + by) % 4, y)
                pairs.append((place(zl, x, y), place(zl ^ flip, *target)))
    return lax.ppermute(array, PLANE, pairs)


def program(acts, grads, damping):
    tokens, width = acts.shape
    nb = width // B
    nz = lax.axis_size("zh")
    scale = 1.0 / (tokens * lax.axis_size(AXES))
    bits = [lax.axis_size(a).bit_length() - 1 for a in AXES]
    shifts = jnp.array([sum(bits[k + 1 :]) for k in range(len(bits))], jnp.int32)
    masks = jnp.array([(1 << b) - 1 for b in bits], jnp.int32)
    at = (lax.axis_index(AXES) >> shifts) & masks
    rings = ("x", Y)
    piece = nb * (nb + 1) // 2 * B // 32
    rows = width // lax.axis_size(DP)
    chunk = (piece, B)
    gram_flops = tokens * width * width
    transposed, sent1 = call(
        functools.partial(first_kernel, nb, 1), [at], [acts, grads],
        [jax.ShapeDtypeStruct((2, width, tokens), BF16), (4, 4, *chunk)], flops=gram_flops,
    )

    def factors(colour, which):
        kernel = functools.partial(factor_kernel, nb, colour, which)
        arrays = [acts, grads, transposed]
        return call(kernel, [at], arrays, [(4, 4, *chunk)], flops=gram_flops // 2)[0]

    def crosses_of(which, after):
        shape = (2, 16, nz, rows, B)
        kernel = functools.partial(cross_kernel, nb, which)
        return call(kernel, [at], [grads, transposed], [shape], flops=gram_flops, after=after)[0]

    sent0 = factors(0, 0)
    came = []
    for sent in (sent0, sent1):
        came.append(swapped(sent, "c"))
    near = []
    for colour in range(2):
        near.append([factors(colour, 1), came[colour]])
    sent2 = crosses_of(0, [near[0][0], near[1][0]])
    cross_came = swapped(sent2, "c")
    for depth in range(2):
        far = []
        for colour in range(2):
            axis = depth ^ colour
            turned = call(
                functools.partial(turned_kernel, len(near[colour]), axis), [at],
                near[colour], [chunk if depth else (4, *chunk)] * 4,
            )
            far.append([turned[0]] + [shifted(turned[k], rings[axis], k) for k in (2, 1, 3)])
        near = far
        if depth == 0:
            begun = [near[0][0], near[1][0]]
    cross_kept = crosses_of(1, begun)
    cross_keep, cross_send = call(parted_kernel, [at], [cross_kept, cross_came], [(16, nz, rows, B)] * 2)
    cross_came = swapped(cross_send, "zl")
    keep, send = call(halves_kernel, [at], near[0] + near[1], [chunk] * 2)
    arrived = swapped(send, "zl")
    (cross_half,) = call(plus_kernel, [], [cross_keep, cross_came], [(16, nz, rows, B)], after=[send])
    cross_pieces = lax.all_to_all(cross_half, PLANE[1:], 0, 0, tiled=True)
    (half,) = call(total_kernel, [], [keep, arrived], [chunk])
    around = [half] + [shifted(half, "zh", k) for k in (2, 1, 3)]
    (mine,) = call(total_kernel, [], around, [chunk])
    (cross_sum,) = call(summed_kernel, [], [cross_pieces], [(nz, rows, B)])
    other = {k: sent_across(mine, k, 1, 0) for k in (2, 1, 3, 0)}
    same = {k: sent_across(mine, k, 0, 0) for k in (2, 1, 3)}
    joined = call(
        joined_kernel, [at], [mine, *(same[k] for k in (1, 2, 3)), *(other[k] for k in range(4))],
        [(4, piece, B)] * 2,
    )
    cross_parts = lax.all_to_all(cross_sum, "zh", 0, 0, tiled=True)
    spread = ("zh", "x", "yh")
    (sent_rows,) = call(
        functools.partial(repeated_kernel, scale), [], [cross_parts],
        [(lax.axis_size(spread), rows, B)],
    )
    moved = {}
    for steps in ((2,), (1, 3)):
        for colour in range(2):
            for k in steps:
                moved[colour, k] = shifted(joined[colour], rings[colour], k)
    pieces = []
    for colour in range(2):
        pieces += [joined[colour]] + [moved[colour, k] for k in (1, 2, 3)]
    cross_rows = lax.all_to_all(sent_rows, spread, 0, 0, tiled=True)
    (mine,) = call(
        functools.partial(inverse_kernel, nb, scale), [at, damping], pieces,
        [(B, width)],
        [
            pltpu.VMEM((32, piece, B), F32),
            pltpu.VMEM((width, width), F32),
            pltpu.VMEM((width, width), BF16),
            pltpu.VMEM((width, width), BF16),
            pltpu.VMEM((B, width), F32),
            pltpu.VMEM((B, width), F32),
        ],
        flops=2 * 3 * STEPS * B * width * width,
        limit=24,
    )
    other = swapped(mine, "c")
    (z,) = call(rows_kernel, [at], [cross_rows, mine, other], [(nz, rows, B)], [pltpu.VMEM((nz * rows, width), F32)])
    slabs = [z, swapped(z, "yl"), swapped(z, "zl"), swapped(z, ("zl", "yl"))]
    came = swapped(jnp.stack(slabs), "c")
    (out,) = call(
        last_kernel, [at], [mine, other, *slabs, came], [(rows, B)],
        [pltpu.VMEM((2, 2, nz, 2, rows, B), F32)],
    )
    return out


def solution(mesh):
    torus = Mesh(mesh.devices.reshape(4, 2, 2, 2, 4, 2), AXES)
    return jax.shard_map(
        program,
        mesh=torus,
        in_specs=(P(AXES, None), P(AXES, None), P()),
        out_specs=P(DP, GRP),
        check_vma=False,
    )
```
